32 devices in a mesh: row: 8 (over y, x, core), col: 4 (over z).
Axes of the slice: x: 2, y: 2, z: 4, core: 2. Of those that a mesh axis runs over, the one named last changes fastest.
Arguments:
- vectors: float32 [32768, 4096], P('row', 'col'), may hold values from -6 to 6
- reflectors: float32 [8, 32768, 128], P('col', 'row'), may hold values from -0.03125 to 0.03125
- triangles: float32 [8, 128, 128], P('col'), may hold values from -0.25 to 1.8, as said below
Outputs:
- transformed: float32 [32768, 4096], P('row', 'col')
The draws below stay inside these ranges and needn't reach their ends.
Inputs may be any that keep to these rules, and one draw needn't show every extreme that they name: Each triangles[p] is upper triangular with diagonal entries between 0.5 and 1.8.
All inputs are finite; a program needn't handle non-finite values.
Results may differ from the reference program's by a relative error of at most 0.00013.
Values sent between devices are 32-bit elements; how exact they have to be, the bound alone decides.
A program may use at most 128 MiB of HBM per device.

```python
import jax
import jax.numpy as jnp
from jax import lax

ORDER = 32768
NB = 128
PANELS = 8
COLS = 4096


def draw_triangles(key, part):
    first, second = jax.random.split(jax.random.fold_in(key, 7))
    diagonal = jax.random.uniform(first, (PANELS, NB), jnp.float32, 0.5, 1.5)
    offdiag = jnp.clip(0.05 * jax.random.normal(second, (PANELS, NB, NB), jnp.float32), -0.25, 0.25)
    ident = jnp.eye(NB, dtype=jnp.float32)
    return jnp.triu(offdiag, 1) + diagonal[:, :, None] * ident[None, :, :]


def level_of(rng, shape, cuts, low, largest):
    def one(axis_at, shards_of):
        steps = jax.random.uniform(jax.random.fold_in(jax.random.fold_in(rng, 6), axis_at), (shards_of,), jnp.float32, low / len(cuts), largest / len(cuts))
        return jnp.repeat(jnp.exp(steps), shape[axis_at] // shards_of).reshape((-1,) + (1,) * (len(shape) - axis_at - 1))

    gain = one(*cuts[0])
    for cut in cuts[1:]:
        gain = gain * one(*cut)
    return gain


def noise(own_key, extent, scale, bound, shards=(), kind=jnp.bfloat16):
    result = scale * jax.random.normal(own_key, extent, jnp.float32)
    if shards:
        result = result * level_of(own_key, extent, shards, -0.22, 0.18)
    return jnp.clip(result, -bound, bound).astype(kind)


def setup_inputs(seed: int = 0) -> dict:
    key_list = jax.random.split(jax.random.key(seed), 4)
    vectors = noise(key_list[0], (ORDER, COLS), 1.0, 6.0, ((0, 8), (1, 4)), jnp.float32)
    reflectors = noise(key_list[1], (PANELS, ORDER, NB), ORDER ** -0.5, 0.03125, ((0, 4), (1, 8)), jnp.float32)
    triangles = draw_triangles(jax.random.fold_in(key_list[3], 71), 0)
    return dict(vectors=vectors, reflectors=reflectors, triangles=triangles)


def reference(vectors, reflectors, triangles):
    hi = lax.Precision.HIGHEST
    block = vectors
    for panel in range(PANELS - 1, -1, -1):
        basis = reflectors[panel]
        summed = lax.dot_general(basis, block, (((0,), (0,)), ((), ())), precision=hi, preferred_element_type=jnp.float32)
        scaled = jnp.dot(triangles[panel], summed, precision=hi, preferred_element_type=jnp.float32)
        block = block - jnp.dot(basis, scaled, precision=hi, preferred_element_type=jnp.float32)
    return block
```

```python
import functools

import jax
import jax.numpy as jnp
from jax import lax
from jax.experimental import pallas as pl
from jax.experimental.pallas import tpu as pltpu
from jax.sharding import PartitionSpec as P

F32, BF16 = jnp.float32, jnp.bfloat16
MESH = pl.DeviceIdType.MESH
VMEM_BYTES = 67043328
CHUNK = 256


def split(value):
    high = value.astype(BF16)
    return high, (value - high.astype(F32)).astype(BF16)


def dot(left, right):
    return jnp.dot(left, right, preferred_element_type=F32)


def exact(left, right):
    return jnp.dot(left, right, precision=lax.Precision.HIGHEST, preferred_element_type=F32)


class Line:
    def __init__(self, n, per_dev):
        self.n, self.per_dev = n, per_dev
        self.first = per_dev - per_dev // 2
        self.last = per_dev - self.first

    def below(self, z, q):
        return self.per_dev * z - 1 - q

    def above(self, z, q):
        n, first, last = self.n, self.first, self.last
        lead = (n - 1 - z) * first
        outward = self.per_dev * (z + 1 + q // first) + self.per_dev - 1 - q % first
        if not last:
            return outward
        rest = q - lead
        inward = self.per_dev * (n - 1 - rest // last) + last - 1 - rest % last
        if isinstance(z, int):
            return outward if q < lead else inward
        return jnp.where(q < lead, outward, inward)

    def needed(self, z, panel):
        owner = panel // self.per_dev
        if owner == z:
            return 0
        if owner < z:
            return 2 * (self.per_dev * z - panel)
        order = [self.above(z, q) for q in range(self.per_dev * (self.n - 1 - z))]
        return 2 * (order.index(panel) + 1)


def groups_of(panels):
    final = max(1, 3 * panels // 8)
    middle = min(panels - final, 3 * panels // 8)
    groups = []
    for low, high in ((final + middle, panels), (final, final + middle)):
        if high > low:
            order = [high - 1, *range(low, high - 1)]
            groups.append((order, order))
    groups.append(([*range(final - 2, -1, -1), final - 1], [*range(final - 1, -1, -1)]))
    return groups


def kernel(n, g, groups, x_in, v_in, t_in, x_out, v_out, y_out,
           X, V, T, acc, pair, half, parts, red, yb,
           local_sem, up_send, up_recv, dn_send, dn_recv, tz_send, tz_recv, tr_send, tr_recv,
           a_send, a_recv, b_send, b_recv, c_send, c_recv, d_send, d_recv):
    panels, rows, nb = V.shape
    per_dev = v_in.shape[0]
    cols = X.shape[1]
    unit = rows // 2
    line = Line(n, per_dev)
    chips = g // 2
    z, me = lax.axis_index("col"), lax.axis_index("row")
    core, chip = lax.rem(me, 2), lax.div(me, 2)
    partner = me + 1 - 2 * core
    quarter = nb // g

    barrier = pltpu.get_barrier_semaphore()
    for d in range(1, g):
        pl.semaphore_signal(barrier, inc=1, device_id={"row": lax.rem(me + d, g)}, device_id_type=MESH)
    for d in range(1, n):
        pl.semaphore_signal(barrier, inc=1, device_id={"col": lax.rem(z + d, n)}, device_id_type=MESH)
    pl.semaphore_wait(barrier, g - 1 + n - 1)

    def remote(src, dst, send, recv, where):
        return pltpu.make_async_remote_copy(
            src_ref=src, dst_ref=dst, send_sem=send, recv_sem=recv, device_id=where, device_id_type=MESH
        )

    def piece(panel, at):
        return V.at[panel, pl.ds(at * unit, unit)]

    def own(j, at):
        return v_in.at[j, pl.ds(at * unit, unit)]

    def up(k, src, dst):
        return remote(src, dst, up_send.at[k], up_recv.at[k], {"col": lax.rem(z + 1, n)})

    def down(k, src, dst):
        return remote(src, dst, dn_send.at[k], dn_recv.at[k], {"col": lax.rem(z + n - 1, n)})

    def send_last():
        for i in range(2 * line.last):
            j = line.last - 1 - i // 2
            down(2 * (line.first + per_dev * (n - 1 - z)) + i, own(j, i % 2), piece(per_dev * z + j, i % 2)).start()

    @pl.when(z < n - 1)
    def _():
        for k in range(2 * per_dev):
            j = per_dev - 1 - k // 2
            up(k, own(j, k % 2), piece(per_dev * z + j, k % 2)).start()

    @pl.when(z > 0)
    def _():
        for k in range(2 * line.first):
            j = per_dev - 1 - k // 2
            down(k, own(j, k % 2), piece(per_dev * z + j, k % 2)).start()

    @pl.when(z == n - 1)
    def _():
        send_last()

    mine = pl.ds(me * quarter, quarter)
    owned = pl.ds(z * per_dev, per_dev)
    t_own = pltpu.make_async_copy(t_in.at[:, mine], T.at[owned, mine], local_sem.at[0])
    t_own.start()
    t_across = [
        remote(t_in.at[:, mine], T.at[owned, mine], tz_send.at[d - 1], tz_recv.at[d - 1], {"col": lax.rem(z + d, n)})
        for d in range(1, n)
    ]
    for copy in t_across:
        copy.start()
    v_own = pltpu.make_async_copy(v_in, V.at[owned], local_sem.at[1])
    v_own.start()
    x_load = pltpu.make_async_copy(x_in, X, local_sem.at[2])
    x_load.start()
    t_own.wait()
    for copy in t_across:
        copy.wait()
    t_along = [
        remote(T.at[:, mine], T.at[:, mine], tr_send.at[d - 1], tr_recv.at[d - 1], {"row": lax.rem(me + d, g)})
        for d in range(1, g)
    ]
    for copy in t_along:
        copy.start()
    v_own.wait()
    x_load.wait()
    for copy in t_along:
        copy.wait()

    def service(u):
        q, at = u // 2, u % 2

        @pl.when(u < 2 * per_dev * z)
        def _():
            spot = piece(line.below(z, q), at)
            up(u, spot, spot).wait_recv()

            @pl.when(z < n - 1)
            def _():
                if u + 2 * per_dev < 2 * per_dev * (n - 1):
                    up(u + 2 * per_dev, spot, spot).start()

        @pl.when(u < 2 * per_dev * (n - 1 - z))
        def _():
            spot = piece(line.above(z, q), at)
            down(u, spot, spot).wait_recv()

            @pl.when(z > 0)
            def _():
                if u + 2 * line.first < 2 * per_dev * (n - 1):
                    down(u + 2 * line.first, spot, spot).start()

            if line.last:

                @pl.when((z > 0) & (u == 2 * per_dev * (n - 1 - z) - 1))
                def _():
                    send_last()

    served = [0]

    def ensure(count):
        for u in range(served[0], count):
            service(u)
        served[0] = max(served[0], count)

    def clear(s, width):
        acc[s, :, pl.ds(0, width)] = jnp.zeros((nb, width), F32)

    def product(s, panel, before, start, count):
        width = cols + nb * len(before)

        @pl.loop(0, count // CHUNK)
        def _(i):
            span = pl.ds(pl.multiple_of(start + i * CHUNK, CHUNK), CHUNK)
            high, low = split(V[panel, span, :].T)
            right = jnp.concatenate([X[span, :]] + [V[b, span, :] for b in before], axis=1)
            right_high, right_low = split(right)
            both = dot(jnp.concatenate([high, low], axis=0), right_high)
            acc[s, :, pl.ds(0, width)] += both[:nb] + both[nb:] + dot(high, right_low)

    top = nb // 2
    tall = top // chips

    def sum_a(s, width):
        cut = pl.ds(0, width)
        remote(acc.at[s, pl.ds(top * (1 - core), top), cut], pair.at[s, :, cut], a_send.at[s], a_recv.at[s], {"row": partner}).start()

    def sum_b(s, width):
        cut = pl.ds(0, width)
        kept = acc.at[s, pl.ds(top * core, top), cut]
        remote(kept, pair.at[s, :, cut], a_send.at[s], a_recv.at[s], {"row": partner}).wait()
        half[s, :, cut] = kept[...] + pair[s, :, cut]
        for d in range(1, chips):
            other = lax.rem(chip + d, chips)
            remote(
                half.at[s, pl.ds(other * tall, tall), cut], parts.at[s, d - 1, :, cut],
                b_send.at[s, d - 1], b_recv.at[s, d - 1], {"row": 2 * other + core},
            ).start()

    def sum_c(s, width):
        cut = pl.ds(0, width)
        here = half.at[s, pl.ds(chip * tall, tall), cut]
        total = here[...]
        for d in range(1, chips):
            other = lax.rem(chip + d, chips)
            remote(here, parts.at[s, d - 1, :, cut], b_send.at[s, d - 1], b_recv.at[s, d - 1], {"row": 2 * other + core}).wait()
            total = total + parts[s, d - 1, :, cut]
        spot = red.at[s, pl.ds(top * core + chip * tall, tall), cut]
        spot[...] = total
        for d in range(1, chips):
            other = lax.rem(chip + d, chips)
            remote(spot, spot, c_send.at[s, d - 1], c_recv.at[s, d - 1], {"row": 2 * other + core}).start()

    def sum_d(s, width):
        cut = pl.ds(0, width)
        for d in range(1, chips):
            source = lax.rem(chip + chips - d, chips)
            spot = red.at[s, pl.ds(top * core + source * tall, tall), cut]
            remote(spot, spot, c_send.at[s, d - 1], c_recv.at[s, d - 1], {"row": 2 * source + core}).wait()
        spot = red.at[s, pl.ds(top * core, top), cut]
        remote(spot, spot, d_send.at[s], d_recv.at[s], {"row": partner}).start()

    def sum_e(s, width):
        cut = pl.ds(0, width)
        spot = red.at[s, pl.ds(top * (1 - core), top), cut]
        remote(spot, spot, d_send.at[s], d_recv.at[s], {"row": partner}).wait()

    steps = [sum_a, sum_b, sum_c, sum_d, sum_e]

    def solve(base, order, low, store):
        solved = {}
        for panel in sorted(order, reverse=True):
            at = order.index(panel)
            value = red[base + at, :, pl.ds(0, cols)]
            for later in solved:
                behind = order.index(later)
                if at > behind:
                    gram = red[base + at, :, pl.ds(cols + nb * behind, nb)]
                else:
                    gram = red[base + behind, :, pl.ds(cols + nb * at, nb)].T
                value = value - exact(gram, solved[later])
            solved[panel] = exact(T[panel], value)
            store(panel - low, solved[panel])

    base = 0
    for index, (near, far) in enumerate(groups):
        count, low = len(near), min(near)
        size = nb * count
        if index == len(groups) - 1:
            save = pltpu.make_async_copy(X, x_out, local_sem.at[0])
            save.start()
        pending = []

        def advance():
            for item in pending:
                steps[item[2]](item[0], item[1])
                item[2] += 1
            pending[:] = [item for item in pending if item[2] < len(steps)]

        done = []
        for k in range(count):
            panel = near[k] if near[k] == far[k] else jnp.where(z < n // 2, near[k], far[k])
            wait = max(
                line.needed(place, near[k] if place < n // 2 else far[k]) for place in range(n)
            )
            width = cols + nb * k
            clear(base + k, width)
            if index == len(groups) - 1 and k == count - 1:
                ensure(wait - 1)
                product(base + k, panel, done, 0, unit)
                ensure(2 * per_dev * (n - 1))
                product(base + k, panel, done, unit, unit)
            else:
                ensure(wait)
                product(base + k, panel, done, 0, rows)
            if index == len(groups) - 1:
                pltpu.make_async_copy(V.at[panel], v_out.at[:, pl.ds(pl.multiple_of((panel - low) * nb, nb), nb)], local_sem.at[1 + k]).start()
            pending.append([base + k, width, 0])
            advance()
            done.append(panel)
        while pending:
            advance()

        if index < len(groups) - 1:

            def store(at, value):
                high, rest = split(value)
                yb[pl.ds(at * nb, nb), :] = high
                yb[pl.ds(size + at * nb, nb), :] = high
                yb[pl.ds(2 * size + at * nb, nb), :] = rest

            solve(base, near, low, store)

            @pl.loop(0, rows // CHUNK)
            def _(i):
                span = pl.ds(pl.multiple_of(i * CHUNK, CHUNK), CHUNK)
                high, rest = split(jnp.concatenate([V[low + p, span, :] for p in range(count)], axis=1))
                X[span, :] -= dot(jnp.concatenate([high, rest, high], axis=1), yb[pl.ds(0, 3 * size), :])
        else:

            def store(at, value):
                y_out[pl.ds(at * nb, nb), :] = value

            @pl.when(z < n // 2)
            def _():
                solve(base, near, low, store)

            @pl.when(z >= n // 2)
            def _():
                solve(base, far, low, store)

            save.wait()
            for k in range(count):
                panel = jnp.where(z < n // 2, near[k], far[k])
                pltpu.make_async_copy(V.at[panel], v_out.at[:, pl.ds(pl.multiple_of((panel - low) * nb, nb), nb)], local_sem.at[1 + k]).wait()
        base += count

    for k in range(2 * per_dev * (n - 1)):

        @pl.when((z < n - 1) & (k < 2 * per_dev * (z + 1)))
        def _():
            up(k, piece(0, 0), piece(0, 0)).wait_send()

        @pl.when((z > 0) & (k < 2 * per_dev * (n - z)))
        def _():
            down(k, piece(0, 0), piece(0, 0)).wait_send()


def shards(n, g, vectors, reflectors, triangles):
    per_dev, rows, nb = reflectors.shape
    cols = vectors.shape[1]
    panels = per_dev * n
    groups = groups_of(panels)
    most = max(len(near) for near, _ in groups)
    final = len(groups[-1][0])
    wide = cols + nb * (most - 1)
    chips = g // 2
    sems = pltpu.SemaphoreType.DMA
    anywhere = pl.BlockSpec(memory_space=pl.ANY)
    ends = 2 * per_dev * (n - 1)
    peers = max(1, chips - 1)
    early, basis, scaled = pl.pallas_call(
        functools.partial(kernel, n, g, groups),
        out_shape=(
            jax.ShapeDtypeStruct((rows, cols), F32),
            jax.ShapeDtypeStruct((rows, nb * final), F32),
            jax.ShapeDtypeStruct((nb * final, cols), F32),
        ),
        in_specs=[anywhere] * 3,
        out_specs=(anywhere, anywhere, pl.BlockSpec(memory_space=pltpu.VMEM)),
        scratch_shapes=[
            pltpu.VMEM((rows, cols), F32),
            pltpu.VMEM((panels, rows, nb), F32),
            pltpu.VMEM((panels, nb, nb), F32),
            pltpu.VMEM((panels, nb, wide), F32),
            pltpu.VMEM((panels, nb // 2, wide), F32),
            pltpu.VMEM((panels, nb // 2, wide), F32),
            pltpu.VMEM((panels, peers, nb // 2 // chips, wide), F32),
            pltpu.VMEM((panels, nb, wide), F32),
            pltpu.VMEM((3 * nb * most, cols), BF16),
            sems((max(3, 1 + final),)),
            sems((ends,)), sems((ends,)), sems((ends,)), sems((ends,)),
            sems((n - 1,)), sems((n - 1,)), sems((g - 1,)), sems((g - 1,)),
            sems((panels,)), sems((panels,)),
            sems((panels, peers)), sems((panels, peers)), sems((panels, peers)), sems((panels, peers)),
            sems((panels,)), sems((panels,)),
        ],
        compiler_params=pltpu.CompilerParams(
            collective_id=0, has_side_effects=True, vmem_limit_bytes=VMEM_BYTES
        ),
    )(vectors, reflectors, triangles)
    return early - jnp.dot(basis, scaled, precision=lax.Precision.HIGH, preferred_element_type=F32)


def solution(mesh):
    n, g = mesh.shape["col"], mesh.shape["row"]
    placed = (P("row", "col"), P("col", "row", None), P("col", None, None))
    return jax.shard_map(
        functools.partial(shards, n, g), mesh=mesh, in_specs=placed, out_specs=P("row", "col"), check_vma=False
    )
```

```python
import functools

import jax
import jax.numpy as jnp
from jax import lax
from jax.experimental import pallas as pl
from jax.experimental.pallas import tpu as pltpu
from jax.sharding import PartitionSpec as P

F32, BF16 = jnp.float32, jnp.bfloat16
MESH = pl.DeviceIdType.MESH
VMEM_BYTES = 67043328
CHUNK = 512
STEP = 512
LAST = 512


def split(value):
    high = value.astype(BF16)
    return high, (value - high.astype(F32)).astype(BF16)


def dot(left, right):
    return jnp.dot(left, right, preferred_element_type=F32)


def exact(left, right):
    left_high, left_low = split(left)
    right_high, right_low = split(right)
    return dot(
        jnp.concatenate([left_high, left_low, left_high], axis=1),
        jnp.concatenate([right_high, right_high, right_low], axis=0),
    )


class Line:
    def __init__(self, n, per_dev):
        self.n, self.per_dev = n, per_dev
        self.first = per_dev - per_dev // 2
        self.last = per_dev - self.first

    def below(self, z, q):
        return self.per_dev * z - 1 - q

    def above(self, z, q):
        n, first, last = self.n, self.first, self.last
        lead = (n - 1 - z) * first
        outward = self.per_dev * (z + 1 + q // first) + self.per_dev - 1 - q % first
        if not last:
            return outward
        rest = q - lead
        inward = self.per_dev * (n - 1 - rest // last) + last - 1 - rest % last
        if isinstance(z, int):
            return outward if q < lead else inward
        return jnp.where(q < lead, outward, inward)

    def needed(self, z, panel):
        owner = panel // self.per_dev
        if owner == z:
            return 0
        if owner < z:
            return 2 * (self.per_dev * z - panel)
        order = [self.above(z, q) for q in range(self.per_dev * (self.n - 1 - z))]
        return 2 * (order.index(panel) + 1)


class Plan:
    def __init__(self, panels):
        self.final = max(1, 3 * panels // 8)
        low = self.final
        self.first = [low, low + 2, *range(panels - 1, low + 2, -1)]
        self.chosen = [*range(low + 2, panels)]
        self.near = [*range(low - 2, -1, -1), low - 1]
        self.far = [*range(low - 1, -1, -1)]
        self.grams = max(len(self.first) - 1, low)
        self.update = max(len(self.chosen), low)


def kernel(n, g, plan, x_in, v_in, t_in, x_out, v_out, y_out,
           X, V, T, acc, pair, half, parts, red, yb, Y,
           local_sem, up_send, up_recv, dn_send, dn_recv, tz_send, tz_recv, tr_send, tr_recv,
           a_send, a_recv, b_send, b_recv, c_send, c_recv, d_send, d_recv):
    panels, rows, nb = V.shape
    per_dev = v_in.shape[0]
    cols = X.shape[1]
    unit = rows // 2
    line = Line(n, per_dev)
    chips = g // 2
    z, me = lax.axis_index("col"), lax.axis_index("row")
    core, chip = lax.rem(me, 2), lax.div(me, 2)
    partner = me + 1 - 2 * core
    quarter = nb // g

    barrier = pltpu.get_barrier_semaphore()
    for d in range(1, g):
        pl.semaphore_signal(barrier, inc=1, device_id={"row": lax.rem(me + d, g)}, device_id_type=MESH)
    for d in range(1, n):
        pl.semaphore_signal(barrier, inc=1, device_id={"col": lax.rem(z + d, n)}, device_id_type=MESH)
    pl.semaphore_wait(barrier, g - 1 + n - 1)

    def remote(src, dst, send, recv, where):
        return pltpu.make_async_remote_copy(
            src_ref=src, dst_ref=dst, send_sem=send, recv_sem=recv, device_id=where, device_id_type=MESH
        )

    def piece(panel, at):
        return V.at[panel, pl.ds(at * unit, unit)]

    def own(j, at):
        return v_in.at[j, pl.ds(at * unit, unit)]

    def up(k, src, dst):
        return remote(src, dst, up_send.at[k], up_recv.at[k], {"col": lax.rem(z + 1, n)})

    def down(k, src, dst):
        return remote(src, dst, dn_send.at[k], dn_recv.at[k], {"col": lax.rem(z + n - 1, n)})

    def send_last():
        for i in range(2 * line.last):
            j = line.last - 1 - i // 2
            down(2 * (line.first + per_dev * (n - 1 - z)) + i, own(j, i % 2), piece(per_dev * z + j, i % 2)).start()

    @pl.when(z < n - 1)
    def _():
        for k in range(2 * per_dev):
            j = per_dev - 1 - k // 2
            up(k, own(j, k % 2), piece(per_dev * z + j, k % 2)).start()

    @pl.when(z > 0)
    def _():
        for k in range(2 * line.first):
            j = per_dev - 1 - k // 2
            down(k, own(j, k % 2), piece(per_dev * z + j, k % 2)).start()

    @pl.when(z == n - 1)
    def _():
        send_last()

    mine = pl.ds(me * quarter, quarter)
    owned = pl.ds(z * per_dev, per_dev)
    t_own = pltpu.make_async_copy(t_in.at[:, mine], T.at[owned, mine], local_sem.at[0])
    t_own.start()
    t_across = [
        remote(t_in.at[:, mine], T.at[owned, mine], tz_send.at[d - 1], tz_recv.at[d - 1], {"col": lax.rem(z + d, n)})
        for d in range(1, n)
    ]
    for copy in t_across:
        copy.start()
    t_along = [
        remote(T.at[:, mine], T.at[:, mine], tr_send.at[d - 1], tr_recv.at[d - 1], {"row": lax.rem(me + d, g)})
        for d in range(1, g)
    ]
    v_own = pltpu.make_async_copy(v_in, V.at[owned], local_sem.at[1])
    x_load = pltpu.make_async_copy(x_in, X, local_sem.at[2])

    def service(u):
        q, at = u // 2, u % 2

        @pl.when(u < 2 * per_dev * z)
        def _():
            spot = piece(line.below(z, q), at)
            up(u, spot, spot).wait_recv()

            @pl.when(z < n - 1)
            def _():
                if u + 2 * per_dev < 2 * per_dev * (n - 1):
                    up(u + 2 * per_dev, spot, spot).start()

        @pl.when(u < 2 * per_dev * (n - 1 - z))
        def _():
            spot = piece(line.above(z, q), at)
            down(u, spot, spot).wait_recv()

            @pl.when(z > 0)
            def _():
                if u + 2 * line.first < 2 * per_dev * (n - 1):
                    down(u + 2 * line.first, spot, spot).start()

            if line.last:

                @pl.when((z > 0) & (u == 2 * per_dev * (n - 1 - z) - 1))
                def _():
                    send_last()

    served = [0]

    def ensure(count):
        for u in range(served[0], count):
            with jax.named_scope(f"hop{u}"):
                service(u)
        served[0] = max(served[0], count)

    slots = acc.shape[0]

    def product(s, panel, before, start, count):
        width = cols + nb * len(before)
        total = acc.at[s % slots, :, pl.ds(0, width)]
        if start == 0:
            total[...] = jnp.zeros((nb, width), F32)

        @pl.loop(0, count // CHUNK)
        def _(i):
            span = pl.ds(pl.multiple_of(start + i * CHUNK, CHUNK), CHUNK)
            high, low = split(V[panel, span, :].T)
            right = jnp.concatenate([X[span, :]] + [V[b, span, :] for b in before], axis=1)
            right_high, right_low = split(right)
            both = dot(jnp.concatenate([high, low], axis=0), right_high)
            total[...] += both[:nb] + both[nb:] + dot(high, right_low)

    top = nb // 2
    tall = top // chips

    def sum_a(s, width):
        cut = pl.ds(0, width)
        remote(acc.at[s % slots, pl.ds(top * (1 - core), top), cut], pair.at[s, :, cut], a_send.at[s], a_recv.at[s], {"row": partner}).start()

    def sum_b(s, width):
        cut = pl.ds(0, width)
        kept = acc.at[s % slots, pl.ds(top * core, top), cut]
        remote(kept, pair.at[s, :, cut], a_send.at[s], a_recv.at[s], {"row": partner}).wait()
        half[s, :, cut] = kept[...] + pair[s, :, cut]
        for d in range(1, chips):
            other = lax.rem(chip + d, chips)
            remote(
                half.at[s, pl.ds(other * tall, tall), cut], parts.at[s, d - 1, :, cut],
                b_send.at[s, d - 1], b_recv.at[s, d - 1], {"row": 2 * other + core},
            ).start()

    def sum_c(s, width):
        cut = pl.ds(0, width)
        here = half.at[s, pl.ds(chip * tall, tall), cut]
        total = here[...]
        for d in range(1, chips):
            other = lax.rem(chip + d, chips)
            remote(here, parts.at[s, d - 1, :, cut], b_send.at[s, d - 1], b_recv.at[s, d - 1], {"row": 2 * other + core}).wait()
            total = total + parts[s, d - 1, :, cut]
        spot = red.at[s, pl.ds(top * core + chip * tall, tall), cut]
        spot[...] = total
        for d in range(1, chips):
            other = lax.rem(chip + d, chips)
            remote(spot, spot, c_send.at[s, d - 1], c_recv.at[s, d - 1], {"row": 2 * other + core}).start()

    def sum_d(s, width):
        cut = pl.ds(0, width)
        for d in range(1, chips):
            source = lax.rem(chip + chips - d, chips)
            spot = red.at[s, pl.ds(top * core + source * tall, tall), cut]
            remote(spot, spot, c_send.at[s, d - 1], c_recv.at[s, d - 1], {"row": 2 * source + core}).wait()
        spot = red.at[s, pl.ds(top * core, top), cut]
        remote(spot, spot, d_send.at[s], d_recv.at[s], {"row": partner}).start()

    def sum_e(s, width):
        cut = pl.ds(0, width)
        spot = red.at[s, pl.ds(top * (1 - core), top), cut]
        remote(spot, spot, d_send.at[s], d_recv.at[s], {"row": partner}).wait()

    steps = [sum_a, sum_b, sum_c, sum_d, sum_e]

    pending = []

    def step(s):
        for item in pending:
            if item[0] == s:
                with jax.named_scope(f"sum{s}_{item[2]}"):
                    steps[item[2]](s, item[1])
                item[2] += 1
        pending[:] = [item for item in pending if item[2] < len(steps)]

    def advance():
        for item in list(pending):
            step(item[0])

    def drain():
        while pending:
            advance()

    where, places = {}, {}

    def form(name, before, wait, wait_half, between):
        s, panel, behind = len(where), index_of(name), [index_of(b) for b in before]
        with jax.named_scope(f"wait{s}"):
            ensure(wait_half)
        with jax.named_scope(f"product{s}"):
            product(s, panel, behind, 0, unit)
        between()
        with jax.named_scope(f"wait{s}"):
            ensure(wait)
        with jax.named_scope(f"product{s}"):
            product(s, panel, behind, unit, unit)
        pending.append([s, cols + nb * len(before), 0])
        step(s)
        where[name] = s
        places.update({(name, b): (s, at) for at, b in enumerate(before)})

    def index_of(name):
        if not isinstance(name, tuple):
            return name
        near, far = plan.near[name[0]], plan.far[name[0]]
        return near if near == far else jnp.where(z < n // 2, near, far)

    def units_for(name):
        if not isinstance(name, tuple):
            return max(line.needed(place, name) for place in range(n))
        return max(
            line.needed(place, (plan.near if place < n // 2 else plan.far)[name[0]]) for place in range(n)
        )

    def add(name, before, between):
        wait = units_for(name)
        form(name, before, wait, wait, between)

    def gram(a, b):
        if (a, b) in places:
            s, at = places[a, b]
            return red[s, :, pl.ds(cols + nb * at, nb)]
        s, at = places[b, a]
        return red[s, :, pl.ds(cols + nb * at, nb)].T

    def solve(chosen, known, store, names=None):
        names = names or {panel: panel for panel in chosen}
        solved = dict(known)
        for panel in sorted(chosen, reverse=True):
            name = names[panel]
            value = red[where[name], :, pl.ds(0, cols)]
            for later in sorted(solved, reverse=True):
                behind = names.get(later, later)
                if (name, behind) in places or (behind, name) in places:
                    value = value - exact(gram(name, behind), solved[later])
            solved[panel] = exact(T[panel], value)
            store(panel, solved[panel])

    def keep(target, low, size):
        def store(panel, value):
            high, rest = split(value)
            at = (panel - low) * nb
            target[pl.ds(at, nb), :] = high
            target[pl.ds(size + at, nb), :] = high
            target[pl.ds(2 * size + at, nb), :] = rest

        return store

    ensure(1)
    v_own.start()
    x_load.start()
    ensure(2 * per_dev)
    t_own.wait()
    for copy in t_across:
        copy.wait()
    for copy in t_along:
        copy.start()
    v_own.wait()
    x_load.wait()

    def update(low, count):
        size = nb * count

        @pl.loop(0, rows // STEP)
        def _(i):
            span = pl.ds(pl.multiple_of(i * STEP, STEP), STEP)
            high, rest = split(jnp.concatenate([V[low + p, span, :] for p in range(count)], axis=1))
            X[span, :] -= dot(jnp.concatenate([high, rest, high], axis=1), yb[pl.ds(0, 3 * size), :])

    low = plan.final
    last = plan.final - 1
    lent = [low, low + 1]

    def settle(chosen, known):
        put = keep(yb, min(chosen), nb * len(chosen))

        def store(panel, value):
            put(panel, value)
            Y[panel - low] = value

        with jax.named_scope(f"solve{min(chosen)}"):
            solve(chosen, {panel: Y[panel - low] for panel in known}, store)

    for k, panel in enumerate(plan.first):
        add(panel, plan.first[:k], advance)
    drain()
    for copy in t_along:
        copy.wait()
    settle(plan.chosen, [])
    with jax.named_scope("update_chosen"):
        update(low + 2, len(plan.chosen))

    early = [(k,) for k in range(last)]
    formed = [low]
    for name in [*early[:1], low + 1, *early[1:]]:
        add(name, formed, lambda: step(len(where) - 1))
        formed = [*formed, name]
    behind = [where[name] for name in early]

    def nudge():
        for s in behind:
            step(s)

    step(where[low + 1])
    nudge()
    while any(item[0] == where[low + 1] for item in pending):
        step(where[low + 1])
    settle(lent, plan.chosen)
    nudge()
    with jax.named_scope("update_lent"):
        update(low, 2)
    nudge()

    save = pltpu.make_async_copy(X, x_out, local_sem.at[0])
    save.start()
    def give(panel, k):
        spot = v_out.at[:, pl.ds(pl.multiple_of(panel * nb, nb), nb)]
        return pltpu.make_async_copy(V.at[panel], spot, local_sem.at[1 + k])

    ends = 2 * per_dev * (n - 1)

    def prepare():
        drain()
        with jax.named_scope("prepare"):
            for name in early:
                spot = red.at[where[name], :, pl.ds(0, cols)]
                value = spot[...]
                for panel in lent:
                    value = value - exact(gram(name, panel), Y[panel - low])
                spot[...] = value
        for k in range(ends - 2):

            @pl.when((z < n - 1) & (k < 2 * per_dev * (z + 1) - 2))
            def _():
                up(k, piece(0, 0), piece(0, 0)).wait_send()

            @pl.when((z > 0) & (k < 2 * per_dev * (n - z) - 2))
            def _():
                down(k, piece(0, 0), piece(0, 0)).wait_send()

    for k in range(last):
        give(index_of((k,)), k).start()
    form((last,), early, ends, ends - 1, prepare)
    give(index_of((last,)), last).start()
    drain()
    for order, here in ((plan.near, z < n // 2), (plan.far, z >= n // 2)):

        @pl.when(here)
        def _(order=order):
            with jax.named_scope("solve_last"):
                solve(order, {}, keep(y_out, 0, nb * plan.final), {panel: (k,) for k, panel in enumerate(order)})

    save.wait()
    for k in range(plan.final):
        give(index_of((k,)), k).wait()

    for k in range(2):

        @pl.when(z < n - 1)
        def _():
            up(2 * per_dev * (z + 1) - 2 + k, piece(0, 0), piece(0, 0)).wait_send()

        @pl.when(z > 0)
        def _():
            down(2 * per_dev * (n - z) - 2 + k, piece(0, 0), piece(0, 0)).wait_send()


def subtract(x, v, y, out):
    high, rest = split(v[...])
    out[...] = x[...] - dot(jnp.concatenate([high, rest, high], axis=1), y[...])


def shards(n, g, vectors, reflectors, triangles):
    per_dev, rows, nb = reflectors.shape
    cols = vectors.shape[1]
    panels = per_dev * n
    plan = Plan(panels)
    final = plan.final
    wide = cols + nb * plan.grams
    chips = g // 2
    sems = pltpu.SemaphoreType.DMA
    anywhere = pl.BlockSpec(memory_space=pl.ANY)
    ends = 2 * per_dev * (n - 1)
    peers = max(1, chips - 1)
    early, basis, scaled = pl.pallas_call(
        functools.partial(kernel, n, g, plan),
        out_shape=(
            jax.ShapeDtypeStruct((rows, cols), F32),
            jax.ShapeDtypeStruct((rows, nb * final), F32),
            jax.ShapeDtypeStruct((3 * nb * final, cols), BF16),
        ),
        in_specs=[anywhere] * 3,
        out_specs=(anywhere, anywhere, pl.BlockSpec(memory_space=pltpu.VMEM)),
        scratch_shapes=[
            pltpu.VMEM((rows, cols), F32),
            pltpu.VMEM((panels, rows, nb), F32),
            pltpu.VMEM((panels, nb, nb), F32),
            pltpu.VMEM((3, nb, wide), F32),
            pltpu.VMEM((panels, nb // 2, wide), F32),
            pltpu.VMEM((panels, nb // 2, wide), F32),
            pltpu.VMEM((panels, peers, nb // 2 // chips, wide), F32),
            pltpu.VMEM((panels, nb, wide), F32),
            pltpu.VMEM((3 * nb * plan.update, cols), BF16),
            pltpu.VMEM((panels - final, nb, cols), F32),
            sems((max(3, 1 + final),)),
            sems((ends,)), sems((ends,)), sems((ends,)), sems((ends,)),
            sems((n - 1,)), sems((n - 1,)), sems((g - 1,)), sems((g - 1,)),
            sems((panels,)), sems((panels,)),
            sems((panels, peers)), sems((panels, peers)), sems((panels, peers)), sems((panels, peers)),
            sems((panels,)), sems((panels,)),
        ],
        compiler_params=pltpu.CompilerParams(
            collective_id=0, has_side_effects=True, vmem_limit_bytes=VMEM_BYTES
        ),
    )(vectors, reflectors, triangles)
    return pl.pallas_call(
        subtract,
        grid=(rows // LAST,),
        out_shape=jax.ShapeDtypeStruct((rows, cols), F32),
        in_specs=[
            pl.BlockSpec((LAST, cols), lambda i: (i, 0)),
            pl.BlockSpec((LAST, nb * final), lambda i: (i, 0)),
            pl.BlockSpec((3 * nb * final, cols), lambda i: (0, 0)),
        ],
        out_specs=pl.BlockSpec((LAST, cols), lambda i: (i, 0)),
    )(early, basis, scaled)


def solution(mesh):
    n, g = mesh.shape["col"], mesh.shape["row"]
    placed = (P("row", "col"), P("col", "row", None), P("col", None, None))
    return jax.shard_map(
        functools.partial(shards, n, g), mesh=mesh, in_specs=placed, out_specs=P("row", "col"), check_vma=False
    )
```

```python
import functools

import jax
import jax.numpy as jnp
from jax import lax
from jax.experimental import pallas as pl
from jax.experimental.pallas import tpu as pltpu
from jax.sharding import PartitionSpec as P

F32, BF16 = jnp.float32, jnp.bfloat16
MESH = pl.DeviceIdType.MESH
VMEM_BYTES = 67043328
CHUNK = 512
STEP = 512
PIECES = 4
PARTS = 8


def split(value):
    high = value.astype(BF16)
    return high, (value - high.astype(F32)).astype(BF16)


def dot(left, right):
    return jnp.dot(left, right, preferred_element_type=F32)


def exact(left, right):
    left_high, left_low = split(left)
    right_high, right_low = split(right)
    return dot(
        jnp.concatenate([left_high, left_low, left_high], axis=1),
        jnp.concatenate([right_high, right_high, right_low], axis=0),
    )


class Line:
    def __init__(self, n, per_dev):
        self.n, self.per_dev = n, per_dev
        self.first = per_dev - per_dev // 2
        self.last = per_dev - self.first

    def below(self, z, q):
        return self.per_dev * z - 1 - q

    def above(self, z, q):
        n, first, last = self.n, self.first, self.last
        lead = (n - 1 - z) * first
        outward = self.per_dev * (z + 1 + q // first) + self.per_dev - 1 - q % first
        if not last:
            return outward
        rest = q - lead
        inward = self.per_dev * (n - 1 - rest // last) + last - 1 - rest % last
        if isinstance(z, int):
            return outward if q < lead else inward
        return jnp.where(q < lead, outward, inward)

    def needed(self, z, panel):
        owner = panel // self.per_dev
        if owner == z:
            return 0
        if owner < z:
            return PIECES * (self.per_dev * z - panel)
        order = [self.above(z, q) for q in range(self.per_dev * (self.n - 1 - z))]
        return PIECES * (order.index(panel) + 1)


class Plan:
    def __init__(self, panels):
        self.final = max(1, 3 * panels // 8)
        low = self.final
        self.first = [low, low + 2, *range(panels - 1, low + 2, -1)]
        self.chosen = [*range(low + 2, panels)]
        self.near = [*range(low - 2, -1, -1), low - 1]
        self.far = [*range(low - 1, -1, -1)]
        self.grams = max(len(self.first) - 1, low)
        self.update = max(len(self.chosen), low)


def kernel(n, g, plan, x_in, v_in, t_in, x_out, v_out, y_out,
           X, V, T, acc, pair, half, parts, red, yb, Y,
           local_sem, up_send, up_recv, dn_send, dn_recv, tz_send, tz_recv, tr_send, tr_recv,
           a_send, a_recv, b_send, b_recv, c_send, c_recv, d_send, d_recv):
    panels, rows, nb = V.shape
    per_dev = v_in.shape[0]
    cols = X.shape[1]
    unit = rows // PIECES
    line = Line(n, per_dev)
    chips = g // 2
    z, me = lax.axis_index("col"), lax.axis_index("row")
    core, chip = lax.rem(me, 2), lax.div(me, 2)
    partner = me + 1 - 2 * core
    quarter = nb // g

    barrier = pltpu.get_barrier_semaphore()
    for d in range(1, g):
        pl.semaphore_signal(barrier, inc=1, device_id={"row": lax.rem(me + d, g)}, device_id_type=MESH)
    for d in range(1, n):
        pl.semaphore_signal(barrier, inc=1, device_id={"col": lax.rem(z + d, n)}, device_id_type=MESH)
    pl.semaphore_wait(barrier, g - 1 + n - 1)

    def remote(src, dst, send, recv, where):
        return pltpu.make_async_remote_copy(
            src_ref=src, dst_ref=dst, send_sem=send, recv_sem=recv, device_id=where, device_id_type=MESH
        )

    def piece(panel, at):
        return V.at[panel, pl.ds(at * unit, unit)]

    def own(j, at):
        return v_in.at[j, pl.ds(at * unit, unit)]

    def up(k, src, dst):
        return remote(src, dst, up_send.at[k], up_recv.at[k], {"col": lax.rem(z + 1, n)})

    def down(k, src, dst):
        return remote(src, dst, dn_send.at[k], dn_recv.at[k], {"col": lax.rem(z + n - 1, n)})

    def send_last():
        for i in range(PIECES * line.last):
            j = line.last - 1 - i // PIECES
            down(PIECES * (line.first + per_dev * (n - 1 - z)) + i, own(j, i % PIECES), piece(per_dev * z + j, i % PIECES)).start()

    @pl.when(z < n - 1)
    def _():
        for k in range(PIECES * per_dev):
            j = per_dev - 1 - k // PIECES
            up(k, own(j, k % PIECES), piece(per_dev * z + j, k % PIECES)).start()

    @pl.when(z > 0)
    def _():
        for k in range(PIECES * line.first):
            j = per_dev - 1 - k // PIECES
            down(k, own(j, k % PIECES), piece(per_dev * z + j, k % PIECES)).start()

    @pl.when(z == n - 1)
    def _():
        send_last()

    mine = pl.ds(me * quarter, quarter)
    owned = pl.ds(z * per_dev, per_dev)
    t_own = pltpu.make_async_copy(t_in.at[:, mine], T.at[owned, mine], local_sem.at[0])
    t_own.start()
    t_across = [
        remote(t_in.at[:, mine], T.at[owned, mine], tz_send.at[d - 1], tz_recv.at[d - 1], {"col": lax.rem(z + d, n)})
        for d in range(1, n)
    ]
    for copy in t_across:
        copy.start()
    t_along = [
        remote(T.at[:, mine], T.at[:, mine], tr_send.at[d - 1], tr_recv.at[d - 1], {"row": lax.rem(me + d, g)})
        for d in range(1, g)
    ]
    v_own = pltpu.make_async_copy(v_in, V.at[owned], local_sem.at[1])
    x_load = pltpu.make_async_copy(x_in, X, local_sem.at[2])

    def service(u):
        q, at = u // PIECES, u % PIECES

        @pl.when(u < PIECES * per_dev * z)
        def _():
            spot = piece(line.below(z, q), at)
            up(u, spot, spot).wait_recv()

            @pl.when(z < n - 1)
            def _():
                if u + PIECES * per_dev < PIECES * per_dev * (n - 1):
                    up(u + PIECES * per_dev, spot, spot).start()

        @pl.when(u < PIECES * per_dev * (n - 1 - z))
        def _():
            spot = piece(line.above(z, q), at)
            down(u, spot, spot).wait_recv()

            @pl.when(z > 0)
            def _():
                if u + PIECES * line.first < PIECES * per_dev * (n - 1):
                    down(u + PIECES * line.first, spot, spot).start()

            if line.last:

                @pl.when((z > 0) & (u == PIECES * per_dev * (n - 1 - z) - 1))
                def _():
                    send_last()

    served = [0]

    def ensure(count):
        for u in range(served[0], count):
            with jax.named_scope(f"hop{u}"):
                service(u)
        served[0] = max(served[0], count)

    slots = acc.shape[0]

    def product(s, panel, before, start, count):
        width = cols + nb * len(before)
        total = acc.at[s % slots, :, pl.ds(0, width)]
        if start == 0:
            total[...] = jnp.zeros((nb, width), F32)

        @pl.loop(0, count // CHUNK)
        def _(i):
            span = pl.ds(pl.multiple_of(start + i * CHUNK, CHUNK), CHUNK)
            high, low = split(V[panel, span, :].T)
            right = jnp.concatenate([X[span, :]] + [V[b, span, :] for b in before], axis=1)
            right_high, right_low = split(right)
            both = dot(jnp.concatenate([high, low], axis=0), right_high)
            total[...] += both[:nb] + both[nb:] + dot(high, right_low)

    top = nb // 2
    tall = top // chips

    def sum_a(s, start, width, m):
        cut = pl.ds(start, width)
        remote(acc.at[s % slots, pl.ds(top * (1 - core), top), cut], pair.at[s, :, cut], a_send.at[m], a_recv.at[m], {"row": partner}).start()

    def sum_b(s, start, width, m):
        cut = pl.ds(start, width)
        kept = acc.at[s % slots, pl.ds(top * core, top), cut]
        remote(kept, pair.at[s, :, cut], a_send.at[m], a_recv.at[m], {"row": partner}).wait()
        half[s, :, cut] = kept[...] + pair[s, :, cut]
        for d in range(1, chips):
            other = lax.rem(chip + d, chips)
            remote(
                half.at[s, pl.ds(other * tall, tall), cut], parts.at[s, d - 1, :, cut],
                b_send.at[m, d - 1], b_recv.at[m, d - 1], {"row": 2 * other + core},
            ).start()

    def sum_c(s, start, width, m):
        cut = pl.ds(start, width)
        here = half.at[s, pl.ds(chip * tall, tall), cut]
        total = here[...]
        for d in range(1, chips):
            other = lax.rem(chip + d, chips)
            remote(here, parts.at[s, d - 1, :, cut], b_send.at[m, d - 1], b_recv.at[m, d - 1], {"row": 2 * other + core}).wait()
            total = total + parts[s, d - 1, :, cut]
        spot = red.at[s, pl.ds(top * core + chip * tall, tall), cut]
        spot[...] = total
        for d in range(1, chips):
            other = lax.rem(chip + d, chips)
            remote(spot, spot, c_send.at[m, d - 1], c_recv.at[m, d - 1], {"row": 2 * other + core}).start()

    def sum_d(s, start, width, m):
        cut = pl.ds(start, width)
        for d in range(1, chips):
            source = lax.rem(chip + chips - d, chips)
            spot = red.at[s, pl.ds(top * core + source * tall, tall), cut]
            remote(spot, spot, c_send.at[m, d - 1], c_recv.at[m, d - 1], {"row": 2 * source + core}).wait()
        spot = red.at[s, pl.ds(top * core, top), cut]
        remote(spot, spot, d_send.at[m], d_recv.at[m], {"row": partner}).start()

    def sum_e(s, start, width, m):
        cut = pl.ds(start, width)
        spot = red.at[s, pl.ds(top * (1 - core), top), cut]
        remote(spot, spot, d_send.at[m], d_recv.at[m], {"row": partner}).wait()

    steps = [sum_a, sum_b, sum_c, sum_d, sum_e]

    pending = []

    def step(s):
        for item in pending:
            if item[0] == s:
                with jax.named_scope(f"sum{s}_{item[4]}"):
                    steps[item[4]](*item[:4])
                item[4] += 1
        pending[:] = [item for item in pending if item[4] < len(steps)]

    def advance():
        for s in dict.fromkeys(item[0] for item in pending):
            step(s)

    def drain():
        while pending:
            advance()

    where, places = {}, {}

    def form(name, before, wait, wait_half, between, lead=rows // 2, halve=False):
        s, panel, behind = len(where), index_of(name), [index_of(b) for b in before]
        with jax.named_scope(f"wait{s}"):
            ensure(wait_half)
        with jax.named_scope(f"product{s}"):
            product(s, panel, behind, 0, lead)
        between()
        with jax.named_scope(f"wait{s}"):
            ensure(wait)
        with jax.named_scope(f"product{s}"):
            product(s, panel, behind, lead, rows - lead)
        width = cols + nb * len(before)
        part = width // nb // 2 * nb if halve else width
        pending.append([s, 0, part, s, 0])
        if halve:
            pending.append([s, part, width - part, panels, 0])
        step(s)
        where[name] = s
        places.update({(name, b): (s, at) for at, b in enumerate(before)})

    def index_of(name):
        if not isinstance(name, tuple):
            return name
        near, far = plan.near[name[0]], plan.far[name[0]]
        return near if near == far else jnp.where(z < n // 2, near, far)

    def units_for(name):
        if not isinstance(name, tuple):
            return max(line.needed(place, name) for place in range(n))
        return max(
            line.needed(place, (plan.near if place < n // 2 else plan.far)[name[0]]) for place in range(n)
        )

    def add(name, before, between):
        wait = units_for(name)
        form(name, before, wait, wait, between)

    def gram(a, b):
        if (a, b) in places:
            s, at = places[a, b]
            return red[s, :, pl.ds(cols + nb * at, nb)]
        s, at = places[b, a]
        return red[s, :, pl.ds(cols + nb * at, nb)].T

    def solve(chosen, known, store, names=None):
        names = names or {panel: panel for panel in chosen}
        solved = dict(known)
        for panel in sorted(chosen, reverse=True):
            name = names[panel]
            value = red[where[name], :, pl.ds(0, cols)]
            for later in sorted(solved, reverse=True):
                behind = names.get(later, later)
                if (name, behind) in places or (behind, name) in places:
                    value = value - exact(gram(name, behind), solved[later])
            solved[panel] = exact(T[panel], value)
            store(panel, solved[panel])

    def keep(target, low, size, spots=(0, 1, 2)):
        def store(panel, value):
            high, rest = split(value)
            at = (panel - low) * nb
            for k in spots[:-1]:
                target[pl.ds(k * size + at, nb), :] = high
            target[pl.ds(spots[-1] * size + at, nb), :] = rest

        return store

    ensure(1)
    v_own.start()
    x_load.start()
    ensure(PIECES * per_dev)
    t_own.wait()
    for copy in t_across:
        copy.wait()
    for copy in t_along:
        copy.start()
    v_own.wait()
    x_load.wait()

    def update(low, count):
        size = nb * count

        @pl.loop(0, rows // STEP)
        def _(i):
            span = pl.ds(pl.multiple_of(i * STEP, STEP), STEP)
            high, rest = split(jnp.concatenate([V[low + p, span, :] for p in range(count)], axis=1))
            X[span, :] -= dot(jnp.concatenate([high, rest, high], axis=1), yb[pl.ds(0, 3 * size), :])

    low = plan.final
    last = plan.final - 1
    lent = [low, low + 1]

    def settle(chosen, known):
        put = keep(yb, min(chosen), nb * len(chosen))

        def store(panel, value):
            put(panel, value)
            Y[panel - low] = value

        with jax.named_scope(f"solve{min(chosen)}"):
            solve(chosen, {panel: Y[panel - low] for panel in known}, store)

    for k, panel in enumerate(plan.first):
        add(panel, plan.first[:k], advance)
    drain()
    for copy in t_along:
        copy.wait()
    settle(plan.chosen, [])
    with jax.named_scope("update_chosen"):
        update(low + 2, len(plan.chosen))

    early = [(k,) for k in range(last)]
    formed = [low]
    for name in [*early[:1], low + 1, *early[1:]]:
        add(name, formed, lambda: step(len(where) - 1))
        formed = [*formed, name]
    behind = [where[name] for name in early]

    def nudge():
        for s in behind:
            step(s)

    step(where[low + 1])
    nudge()
    while any(item[0] == where[low + 1] for item in pending):
        step(where[low + 1])
    settle(lent, plan.chosen)
    nudge()
    with jax.named_scope("update_lent"):
        update(low, 2)
    nudge()

    save = pltpu.make_async_copy(X, x_out, local_sem.at[0])
    save.start()
    def give(panel, k):
        spot = v_out.at[:, pl.ds(pl.multiple_of(panel * nb, nb), nb)]
        return pltpu.make_async_copy(V.at[panel], spot, local_sem.at[1 + k])

    ends = PIECES * per_dev * (n - 1)

    def prepare():
        drain()
        with jax.named_scope("prepare"):
            for name in early:
                spot = red.at[where[name], :, pl.ds(0, cols)]
                value = spot[...]
                for panel in lent:
                    value = value - exact(gram(name, panel), Y[panel - low])
                spot[...] = value
        for k in range(ends - 2):

            @pl.when((z < n - 1) & (k < PIECES * per_dev * (z + 1) - 2))
            def _():
                up(k, piece(0, 0), piece(0, 0)).wait_send()

            @pl.when((z > 0) & (k < PIECES * per_dev * (n - z) - 2))
            def _():
                down(k, piece(0, 0), piece(0, 0)).wait_send()

    for k in range(last):
        give(index_of((k,)), k).start()
    form((last,), early, ends, ends - 1, prepare, rows - unit, True)
    give(index_of((last,)), last).start()
    drain()
    for order, here in ((plan.near, z < n // 2), (plan.far, z >= n // 2)):

        @pl.when(here)
        def _(order=order):
            with jax.named_scope("solve_last"):
                solve(order, {}, keep(y_out, 0, nb * plan.final, (0, 1)), {panel: (k,) for k, panel in enumerate(order)})

    save.wait()
    for k in range(plan.final):
        give(index_of((k,)), k).wait()

    for k in range(2):

        @pl.when(z < n - 1)
        def _():
            up(PIECES * per_dev * (z + 1) - 2 + k, piece(0, 0), piece(0, 0)).wait_send()

        @pl.when(z > 0)
        def _():
            down(PIECES * per_dev * (n - z) - 2 + k, piece(0, 0), piece(0, 0)).wait_send()


def subtract(sizes, x_in, v_in, y_in, out, X, V, Y, x_sem, v_sem, y_sem, out_sem):
    depth = V.shape[1]
    y_load = pltpu.make_async_copy(y_in, Y, y_sem)
    y_load.start()

    def span(i):
        return pl.ds(sum(sizes[:i]), sizes[i])

    def load(i):
        return (
            pltpu.make_async_copy(x_in.at[span(i)], X.at[span(i)], x_sem.at[i]),
            pltpu.make_async_copy(v_in.at[span(i)], V.at[span(i)], v_sem.at[i]),
        )

    def save(i):
        return pltpu.make_async_copy(X.at[span(i)], out.at[span(i)], out_sem.at[i])

    ahead = 2
    for i in range(ahead):
        for copy in load(i):
            copy.start()
    y_load.wait()
    for i in range(len(sizes)):
        for copy in load(i):
            copy.wait()
        if i + ahead < len(sizes):
            for copy in load(i + ahead):
                copy.start()
        high, rest = split(V[span(i)])
        left = jnp.concatenate([high, rest, high], axis=1)
        right = jnp.concatenate([Y[:depth], Y[:depth], Y[depth:]], axis=0)
        X[span(i)] = X[span(i)] - dot(left, right)
        save(i).start()
    for i in range(len(sizes)):
        save(i).wait()


def shards(n, g, vectors, reflectors, triangles):
    per_dev, rows, nb = reflectors.shape
    cols = vectors.shape[1]
    panels = per_dev * n
    plan = Plan(panels)
    final = plan.final
    wide = cols + nb * plan.grams
    chips = g // 2
    sems = pltpu.SemaphoreType.DMA
    anywhere = pl.BlockSpec(memory_space=pl.ANY)
    ends, sums = PIECES * per_dev * (n - 1), panels + 1
    peers = max(1, chips - 1)
    early, basis, scaled = pl.pallas_call(
        functools.partial(kernel, n, g, plan),
        out_shape=(
            jax.ShapeDtypeStruct((rows, cols), F32),
            jax.ShapeDtypeStruct((rows, nb * final), F32),
            jax.ShapeDtypeStruct((2 * nb * final, cols), BF16),
        ),
        in_specs=[anywhere] * 3,
        out_specs=(anywhere, anywhere, pl.BlockSpec(memory_space=pltpu.VMEM)),
        scratch_shapes=[
            pltpu.VMEM((rows, cols), F32),
            pltpu.VMEM((panels, rows, nb), F32),
            pltpu.VMEM((panels, nb, nb), F32),
            pltpu.VMEM((3, nb, wide), F32),
            pltpu.VMEM((panels, nb // 2, wide), F32),
            pltpu.VMEM((panels, nb // 2, wide), F32),
            pltpu.VMEM((panels, peers, nb // 2 // chips, wide), F32),
            pltpu.VMEM((panels, nb, wide), F32),
            pltpu.VMEM((3 * nb * plan.update, cols), BF16),
            pltpu.VMEM((panels - final, nb, cols), F32),
            sems((max(3, 1 + final),)),
            sems((ends,)), sems((ends,)), sems((ends,)), sems((ends,)),
            sems((n - 1,)), sems((n - 1,)), sems((g - 1,)), sems((g - 1,)),
            sems((sums,)), sems((sums,)),
            sems((sums, peers)), sems((sums, peers)), sems((sums, peers)), sems((sums, peers)),
            sems((sums,)), sems((sums,)),
        ],
        compiler_params=pltpu.CompilerParams(
            collective_id=0, has_side_effects=True, vmem_limit_bytes=VMEM_BYTES
        ),
    )(vectors, reflectors, triangles)
    size = rows // PARTS
    sizes = [size // 2, *[size] * (PARTS - 1), size // 2]
    return pl.pallas_call(
        functools.partial(subtract, sizes),
        out_shape=jax.ShapeDtypeStruct((rows, cols), F32),
        in_specs=[anywhere] * 3,
        out_specs=anywhere,
        scratch_shapes=[
            pltpu.VMEM((rows, cols), F32),
            pltpu.VMEM((rows, nb * final), F32),
            pltpu.VMEM((2 * nb * final, cols), BF16),
            sems((len(sizes),)), sems((len(sizes),)), sems, sems((len(sizes),)),
        ],
        compiler_params=pltpu.CompilerParams(vmem_limit_bytes=VMEM_BYTES),
    )(early, basis, scaled)


def solution(mesh):
    n, g = mesh.shape["col"], mesh.shape["row"]
    placed = (P("row", "col"), P("col", "row", None), P("col", None, None))
    return jax.shard_map(
        functools.partial(shards, n, g), mesh=mesh, in_specs=placed, out_specs=P("row", "col"), check_vma=False
    )
```
